32 devices in a mesh: expert: 8 (over z, x), tensor: 4 (over y, core).
Axes of the slice: x: 2, y: 2, z: 4, core: 2. Of those that a mesh axis runs over, the one named last changes fastest.
Arguments:
- expert_rows: bfloat16 [8, 8, 240, 5120], P('expert', None, None, 'tensor'), may hold values from -6 to 6
- expert_ids: int32 [2048, 6], P('expert'), may hold values from 0 to 39, all different within a row; in each aligned block of 256 rows (0 to 255, 256 to 511, ...) at most 48 rows name the same one
- gate_weights: float32 [2048, 6], P('expert'), may hold values from 0.02 to 0.5
- residual: bfloat16 [2048, 5120], P('expert', 'tensor'), may hold values from -12 to 12
- norm_gain: float32 [5120], P('tensor'), may hold values from 0.1 to 1.9
- down_projection_weight: bfloat16 [5120, 512], P(None, 'tensor'), may hold values from -0.078125 to 0.078125
- latent_norm_gain: float32 [512], replicated, may hold values from 0.1 to 1.9
- up_projection_weight: bfloat16 [512, 32768], P(None, 'tensor'), may hold values from -0.25 to 0.25
Outputs:
- keys_values: bfloat16 [2048, 32768], P('expert', 'tensor')
- attention_input: bfloat16 [2048, 5120], P('expert', 'tensor')
- balance_loss: float32 [], replicated
The draws below stay inside these ranges and needn't reach their ends.
Inputs may be any that keep to these rules, and one draw needn't show every extreme that they name: `expert_ids`: the 6 ids of a token are distinct. Within the 256 rows of one owner (aligned blocks), no expert is named more than 48 times, a bound that some block reaches.
All inputs are finite; a program needn't handle non-finite values.
Results may differ from the reference program's by a relative error of at most 0.0085.
Values may be sent and summed in bfloat16 or wider, within the bound.
No kernel may reach another device: no remote copies, remote signals or barrier semaphores. Data moves between devices by JAX's collectives and lax.ppermute only.
A program may use at most 64 MiB of HBM per device.

```python
import math
import jax
import jax.numpy as jnp
import numpy as np
from jax import lax

MODEL_WIDTH = 5120
LATENT_WIDTH = 512
HEAD_COUNT = 128
HEAD_KEY_PLAIN = 128
HEAD_VALUE = 128
TOP = 6
EXP_DEV = 5
TOK_E = 256
EXPERTS = 40
CAP = 48
SLOTS = 240
TOKENS = 2048
N_EXPERT = 8


def draw_residual(key, part):
    position = jnp.arange(MODEL_WIDTH, dtype=jnp.float32) / (MODEL_WIDTH - 1)
    column_scale = 0.5 * 4.0 ** position
    values_drawn = jnp.clip(jax.random.normal(key, (TOKENS, MODEL_WIDTH), jnp.float32), -6.0, 6.0)
    return (values_drawn * column_scale[None, :]).astype(jnp.bfloat16)


def levels(rng, extent, split, smallest, high):
    gain, own = 1.0, jax.random.fold_in(rng, 6)
    for dim, shards_of in split:
        steps = jnp.exp(jax.random.uniform(jax.random.fold_in(own, dim), (shards_of,), jnp.float32, smallest / len(split), high / len(split)))
        gain = gain * jnp.repeat(steps, extent[dim] // shards_of).reshape([-1 if axis == dim else 1 for axis in range(len(extent))])
    return gain


def deal_out(stream_key, own, number, rows, amount, top, bound, skew):
    sequence = jax.random.permutation(stream_key, amount)
    crowded, usual = portions_of(amount, rows * top, bound, skew, True), portions_of(amount, rows * top, bound, skew, False)
    places = jnp.arange(amount)

    def named(tallies, turn):
        used = int((tallies > 0).sum())
        fixed = max(1, used // 4)
        shifted = fixed + (places - fixed + turn * (used - fixed)) % max(1, amount - fixed)
        return jnp.zeros((amount,), jnp.int32).at[sequence[jnp.where(places < fixed, places, shifted)]].set(jnp.asarray(tallies, jnp.int32))

    tallies = jnp.where(number % 4 == 0, named(crowded, number // 4), named(usual, number - number // 4 - 1))
    mixed = jax.random.permutation(jax.random.fold_in(own, 3), amount)
    donor, taker = mixed[0:amount // 2 * 2:2], mixed[1:amount // 2 * 2:2]
    margin = jnp.minimum(tallies[donor] - 1, bound - tallies[taker]) // 2
    margin = jnp.where((donor == sequence[0]) | (taker == sequence[0]) | (tallies[taker] == 0), 0, jnp.maximum(margin, 0))
    shifted = jax.random.randint(jax.random.fold_in(own, 4), (amount // 2,), 0, 1 << 20) % (margin + 1)
    tallies = tallies.at[donor].add(-shifted).at[taker].add(shifted)
    labels = jnp.searchsorted(jnp.cumsum(tallies), jnp.arange(rows * top), side="right").astype(jnp.int32)
    grid = labels.reshape(top, rows).T
    grid = grid[jax.random.permutation(jax.random.fold_in(own, 1), rows)]
    turn = jax.random.randint(jax.random.fold_in(own, 2), (rows, 1), 0, top)
    return jnp.take_along_axis(grid, (jnp.arange(top)[None, :] + turn) % top, axis=1)


def portions_of(amount, total, bound, skew, full):
    loads = [(1 << 20) // math.isqrt(standing ** skew) + 1 for standing in range(1, amount + 1)]
    largest = bound if full else min(bound, max(-(-total // amount), total * loads[0] // sum(loads)))
    least = 1 if total - largest >= amount - 1 else 0
    given, rest = [largest] + [least] * (amount - 1), total - largest - least * (amount - 1)
    while rest > 0:
        free = [i for i in range(1, amount) if given[i] < largest] or [i for i in range(1, amount) if given[i] < bound]
        whole, budget = sum([loads[i] for i in free]), rest
        for i in free:
            addition = min(bound - given[i], max(1, budget * loads[i] // whole), rest)
            given[i] = given[i] + addition
            rest = rest - addition
    return np.array(given)


def gaussian(stream_key, extent, deviation, most, shards=(), kind=jnp.bfloat16):
    gain = levels(stream_key, extent, shards, -0.22, 0.18) if shards else 1.0
    entries = jax.random.normal(stream_key, extent, jnp.float32) * deviation * gain
    return jnp.minimum(jnp.maximum(entries, -most), most).astype(kind)


def setup_inputs(seed: int = 0) -> dict:
    streams_of = jax.random.split(jax.random.key(seed), 9)
    expert_rows = gaussian(streams_of[0], (N_EXPERT, N_EXPERT, SLOTS, MODEL_WIDTH), 1.0, 6.0, ((0, 8), (3, 4)))
    expert_ids_keys = jax.random.split(jax.random.fold_in(streams_of[1], 1), TOKENS // TOK_E)
    expert_ids_turns = jax.random.permutation(jax.random.fold_in(streams_of[1], 3), TOKENS // TOK_E)
    expert_ids = jax.vmap(lambda own, number: deal_out(jax.random.fold_in(streams_of[1], 2), own, number, TOK_E, EXPERTS, TOP, CAP, 2))(expert_ids_keys, expert_ids_turns).reshape((TOKENS, TOP))
    gate_weights = jnp.clip(jnp.exp(math.log(0.5) - 3.218876 * jax.random.uniform(streams_of[2], (TOKENS, TOP), jnp.float32) ** levels(streams_of[2], (TOKENS, TOP), ((0, 8),), -0.2, 0.2)), 0.02, 0.5)
    residual = draw_residual(jax.random.fold_in(streams_of[8], 71), 0)
    norm_gain = jnp.clip(1.0 + 0.18 * jax.random.normal(streams_of[4], (MODEL_WIDTH,), jnp.float32), 0.1, 1.9)
    down_projection_weight = gaussian(streams_of[5], (MODEL_WIDTH, LATENT_WIDTH), MODEL_WIDTH ** -0.5, 0.078125, ((1, 4),))
    latent_norm_gain = jnp.clip(1.0 + 0.18 * jax.random.normal(streams_of[6], (LATENT_WIDTH,), jnp.float32), 0.1, 1.9)
    up_projection_weight = gaussian(streams_of[7], (LATENT_WIDTH, HEAD_COUNT * (HEAD_KEY_PLAIN + HEAD_VALUE)), LATENT_WIDTH ** -0.5, 0.25, ((1, 4),))
    return {"expert_rows": expert_rows, "expert_ids": expert_ids, "gate_weights": gate_weights, "residual": residual, "norm_gain": norm_gain, "down_projection_weight": down_projection_weight, "latent_norm_gain": latent_norm_gain, "up_projection_weight": up_projection_weight}


EPSILON = 1e-06

def reference(expert_rows, expert_ids, gate_weights, residual, norm_gain, down_projection_weight, latent_norm_gain, up_projection_weight):
    flat = expert_rows.reshape(N_EXPERT * N_EXPERT * SLOTS, MODEL_WIDTH)
    ids = expert_ids.reshape(N_EXPERT, TOK_E, TOP)
    gates = gate_weights.reshape(N_EXPERT, TOK_E, TOP)
    stream_in = residual.reshape(N_EXPERT, TOK_E, MODEL_WIDTH)
    table = jnp.arange(EXPERTS, dtype=jnp.int32)

    def one_owner(inputs):
        owner, ids_block, gate_block, res_block = inputs
        chosen = ids_block[:, :, None] == table[None, None, :]
        hits = lax.optimization_barrier(jnp.sum(chosen.astype(jnp.int32), axis=1)).astype(jnp.int32)
        before = (jnp.cumsum(hits, axis=0) - hits).astype(jnp.int32)
        rank = lax.optimization_barrier(jnp.sum(jnp.where(chosen, before[:, None, :], 0), axis=2)).astype(jnp.int32)
        index = ids_block // EXP_DEV * (N_EXPERT * SLOTS) + owner * SLOTS + ids_block % EXP_DEV * CAP + rank
        picked = jnp.take(flat, index.reshape(-1).astype(jnp.int32), axis=0).reshape(TOK_E, TOP, MODEL_WIDTH).astype(jnp.float32)
        combined = lax.optimization_barrier(jnp.sum(gate_block[:, :, None] * picked, axis=1))
        stream = (res_block.astype(jnp.float32) + combined).astype(jnp.bfloat16)
        stream = lax.optimization_barrier(stream)
        wide = stream.astype(jnp.float32)
        row_scale = lax.rsqrt(lax.optimization_barrier(jnp.mean(wide * wide, axis=1, keepdims=True)) + EPSILON)
        normed = (wide * row_scale * norm_gain[None, :]).astype(jnp.bfloat16)
        latent = jnp.dot(normed, down_projection_weight, preferred_element_type=jnp.float32)
        latent_row_scale = lax.rsqrt(lax.optimization_barrier(jnp.mean(latent * latent, axis=1, keepdims=True)) + EPSILON)
        latent_normed = (latent * latent_row_scale * latent_norm_gain[None, :]).astype(jnp.bfloat16)
        projected = jnp.dot(latent_normed, up_projection_weight, preferred_element_type=jnp.float32).astype(jnp.bfloat16)
        return (projected, normed)
    blocks, normed_blocks = lax.map(one_owner, (jnp.arange(N_EXPERT, dtype=jnp.int32), ids, gates, stream_in))
    keys_values = blocks.reshape(TOKENS, HEAD_COUNT * (HEAD_KEY_PLAIN + HEAD_VALUE))
    attention_input = normed_blocks.reshape(TOKENS, MODEL_WIDTH)
    device_of = expert_ids // EXP_DEV
    hit = (device_of[:, :, None] == jnp.arange(N_EXPERT, dtype=jnp.int32)[None, None, :]).astype(jnp.float32)
    counts = lax.optimization_barrier(jnp.sum(hit, axis=(0, 1)))
    mass = lax.optimization_barrier(jnp.sum(gate_weights[:, :, None] * hit, axis=(0, 1)))
    balance_loss = N_EXPERT * jnp.sum(counts * mass) / (TOP * float(TOKENS) * float(TOKENS))
    return (keys_values, attention_input, balance_loss)
```

```python
import jax
import jax.numpy as jnp
import numpy as np
from jax import lax
from jax.sharding import PartitionSpec as P

TOP = 6
EXP_DEV = 5
EPSILON = 1e-06


def visit_order(nodes):
    return np.array(
        [sorted(range(nodes), key=lambda d: (-abs(d - z), d < z)) for z in range(nodes)], np.int32
    )


def pick(arrays, index):
    value = arrays[0]
    for i in range(1, len(arrays)):
        value = jnp.where(index == i, arrays[i], value)
    return value


def shards(
    expert_rows,
    expert_ids,
    gate_weights,
    residual,
    norm_gain,
    down_projection_weight,
    latent_norm_gain,
    up_projection_weight,
):
    owners = lax.axis_size("expert")
    tensors = lax.axis_size("tensor")
    rows = expert_rows[0]
    slots, width = rows.shape[1:]
    tokens = expert_ids.shape[0]
    capacity = slots // EXP_DEV
    model_width = width * tensors
    lat_cols = down_projection_weight.shape[1]
    latent_width = lat_cols * tensors
    nodes = owners // 2
    me = lax.axis_index("expert")
    x, z = me % 2, me // 2
    shard = lax.axis_index("tensor")
    parts = 2 if width % 256 == 0 else 1
    cols = width // parts
    swap = [(i, i ^ 1) for i in range(owners)]
    order = visit_order(nodes)
    dest = [jnp.asarray(order[:, i])[z] for i in range(nodes)]

    info = jnp.concatenate([expert_ids.astype(jnp.float32).T, gate_weights.T], axis=0)
    infos = [info]
    for k in range(1, nodes):
        shift = [(2 * i + j, 2 * ((i + k) % nodes) + j) for i in range(nodes) for j in range(2)]
        infos.append(lax.ppermute(info, "expert", shift))

    swapped = {}
    for i in range(nodes):
        out = lax.dynamic_index_in_dim(rows, 2 * dest[i] + 1 - x, 0, keepdims=False)
        for h in range(parts):
            swapped[i, h] = lax.ppermute(out[:, h * cols : (h + 1) * cols], "expert", swap)

    blocks = down_projection_weight.reshape(tensors, width, lat_cols)
    held = [lax.dynamic_index_in_dim(blocks, shard, 0, keepdims=False)]
    for k in range(1, tensors):
        out = lax.dynamic_index_in_dim(blocks, (shard + k) % tensors, 0, keepdims=False)
        held.append(
            lax.ppermute(out, "tensor", [(i, (i + k) % tensors) for i in range(tensors)])
        )
    stacked = jnp.stack(held)
    down = jnp.concatenate(
        [
            lax.dynamic_index_in_dim(stacked, (shard - c) % tensors, 0, keepdims=False)
            for c in range(tensors)
        ],
        axis=1,
    )

    lines = jnp.stack(infos)
    line_ids = lines[:, :TOP, :].astype(jnp.int32)
    line_gates = lines[:, TOP:, :]
    device_hit = (
        line_ids[:, :, :, None] // EXP_DEV == jnp.arange(owners, dtype=jnp.int32)
    ).astype(jnp.float32)
    counts = jnp.sum(device_hit, axis=(0, 1, 2))
    mass = jnp.sum(line_gates[:, :, :, None] * device_hit, axis=(0, 1, 2))
    stats = jnp.stack([counts, mass])
    stats = stats + lax.ppermute(stats, "expert", swap)
    total_tokens = float(tokens * owners)
    balance_loss = owners * jnp.sum(stats[0] * stats[1]) / (TOP * total_tokens * total_tokens)

    pair = 2 * EXP_DEV
    names = 2 * EXP_DEV * z + jnp.arange(pair, dtype=jnp.int32)
    column = np.arange(2 * slots)
    expand = jnp.asarray(
        (column[None, :] // capacity == np.arange(pair)[:, None]).astype(np.float32)
    )
    rank_of = jnp.asarray((column % capacity).astype(np.float32))
    earlier = jnp.asarray(np.tril(np.ones((tokens, tokens), np.float32), -1))
    own_first = x == 0

    def matrix(i):
        one = lax.dynamic_index_in_dim(lines, (z - dest[i]) % nodes, 0, keepdims=False)
        ids_t, gates_t = one[:TOP].astype(jnp.int32), one[TOP:]
        eq = (ids_t[:, :, None] == names).astype(jnp.float32)
        hit = jnp.sum(eq, axis=0)
        gate = jnp.sum(eq * gates_t[:, :, None], axis=0)
        before = jnp.dot(earlier, hit)
        key = jnp.where(hit > 0, before, -1.0)
        wide_key, wide_gate = jnp.dot(key, expand), jnp.dot(gate, expand)
        return jnp.where(wide_key == rank_of, wide_gate, 0.0).astype(jnp.bfloat16)

    def combine(i, h, weights):
        mine = lax.dynamic_index_in_dim(rows, 2 * dest[i] + x, 0, keepdims=False)
        mine = mine[:, h * cols : (h + 1) * cols]
        a, b = weights[:, :slots], weights[:, slots:]
        wa, wb = jnp.where(own_first, a, b), jnp.where(own_first, b, a)
        return jnp.dot(wa, mine, preferred_element_type=jnp.float32) + jnp.dot(
            wb, swapped[i, h], preferred_element_type=jnp.float32
        )

    weights = [matrix(i) for i in range(nodes)]
    partial = {
        (i, h): combine(i, h, weights[i]).astype(jnp.bfloat16)
        for i in range(nodes - 1)
        for h in range(parts)
    }

    def position(s, upward):
        table = np.zeros(nodes, np.int32)
        for node in range(nodes):
            d = node + nodes - s if upward else node - nodes + s
            if 0 <= d < nodes:
                table[node] = list(order[node]).index(d)
        return table

    arrived = {}
    for s in range(1, nodes):
        for h in range(parts):
            for upward in (True, False):
                table = position(s, upward)
                top = int(table.max()) + 1
                value = pick([partial[i, h] for i in range(top)], jnp.asarray(table)[z])
                if s > 1:
                    value = (
                        value.astype(jnp.float32) + arrived[h, upward].astype(jnp.float32)
                    ).astype(jnp.bfloat16)
                senders = range(s) if upward else range(nodes - s, nodes)
                step = 1 if upward else -1
                perm = [
                    (2 * i + j, 2 * (i + step) + j)
                    for i in senders
                    for j in range(2)
                    if 0 <= i + step < nodes
                ]
                arrived[h, upward] = lax.ppermute(value, "expert", perm)

    streams = []
    latent_part, squares = 0.0, 0.0
    for h in range(parts):
        piece = slice(h * cols, (h + 1) * cols)
        total = combine(nodes - 1, h, weights[nodes - 1])
        for upward in (True, False):
            if nodes > 1:
                total = total + arrived[h, upward].astype(jnp.float32)
        stream = (residual[:, piece].astype(jnp.float32) + total).astype(jnp.bfloat16)
        wide = stream.astype(jnp.float32)
        squares = squares + jnp.sum(wide * wide, axis=1)
        gained = (wide * norm_gain[None, piece]).astype(jnp.bfloat16)
        latent_part = latent_part + jnp.dot(
            gained, down[piece, :], preferred_element_type=jnp.float32
        )
        streams.append(stream)

    half = tokens // 2
    low = shard % 2 == 0

    def tensor_swap(value, bit):
        return lax.ppermute(value, "tensor", [(i, i ^ bit) for i in range(tensors)])

    bit = 1
    while bit < tensors:
        squares = squares + tensor_swap(squares, bit)
        bit *= 2
    row_scale = lax.rsqrt(squares / model_width + EPSILON)
    top_half, bottom_half = latent_part[:half], latent_part[half:]
    latent = jnp.where(low, top_half, bottom_half) + tensor_swap(
        jnp.where(low, bottom_half, top_half), 1
    )
    bit = 2
    while bit < tensors:
        latent = latent + tensor_swap(latent, bit)
        bit *= 2
    my_scale = jnp.where(low, row_scale[:half], row_scale[half:])[:, None]
    latent = latent * my_scale
    mean = jnp.mean(latent * latent, axis=1, keepdims=True)
    lat_normed = (latent * lax.rsqrt(mean + EPSILON) * latent_norm_gain[None, :]).astype(
        jnp.bfloat16
    )
    other = tensor_swap(lat_normed, 1)
    latent_full = jnp.concatenate(
        [jnp.where(low, lat_normed, other), jnp.where(low, other, lat_normed)], axis=0
    )
    keys_values = jnp.dot(
        latent_full, up_projection_weight, preferred_element_type=jnp.float32
    ).astype(jnp.bfloat16)
    stream = jnp.concatenate(streams, axis=1).astype(jnp.float32)
    normed = (stream * row_scale[:, None] * norm_gain[None, :]).astype(jnp.bfloat16)
    return (keys_values, normed, balance_loss)


def solution(mesh):
    placed = (
        P("expert", None, None, "tensor"),
        P("expert", None),
        P("expert", None),
        P("expert", "tensor"),
        P("tensor"),
        P(None, "tensor"),
        P(),
        P(None, "tensor"),
    )
    return jax.shard_map(
        shards,
        mesh=mesh,
        in_specs=placed,
        out_specs=(P("expert", "tensor"), P("expert", "tensor"), P()),
        check_vma=False,
    )
```

```python
import functools

import jax
import jax.numpy as jnp
import numpy as np
from jax import lax
from jax.experimental import pallas as pl
from jax.experimental.pallas import tpu as pltpu
from jax.sharding import PartitionSpec as P

TOP = 6
EXP_DEV = 5
EPSILON = 1e-06
LANES = 128


f32, bf16 = jnp.float32, jnp.bfloat16


def visit_order(nodes):
    return np.array(
        [sorted(range(nodes), key=lambda d: (-abs(d - z), d < z)) for z in range(nodes)], np.int32
    )


def pick(arrays, index):
    value = arrays[0]
    for i in range(1, len(arrays)):
        value = jnp.where(index == i, arrays[i], value)
    return value


def cost(flops, moved):
    return pl.CostEstimate(flops=int(flops), bytes_accessed=int(moved), transcendentals=0)


def whole(shape):
    return pl.BlockSpec(shape, lambda *_: (0,) * len(shape))


def call(body, scalars, in_specs, out_shapes, operands, estimate, name, grid=(1,), out_specs=None):
    return pl.pallas_call(
        body,
        grid_spec=pltpu.PrefetchScalarGridSpec(
            num_scalar_prefetch=1,
            grid=grid,
            in_specs=in_specs,
            out_specs=out_specs or [whole(o.shape) for o in out_shapes],
        ),
        out_shape=out_shapes,
        cost_estimate=estimate,
        name=name,
        compiler_params=pltpu.CompilerParams(vmem_limit_bytes=40 * 2**20),
    )(scalars, *operands)


def pack_first(parts, cols, at, ids, gates, rows, info, *outs):
    info[:TOP] = ids[...].astype(f32)
    info[TOP:] = gates[...]
    for h in range(parts):
        outs[h][...] = rows[0, :, h * cols : (h + 1) * cols]


def pack_rest(parts, cols, count, at, *refs):
    ins, outs = refs[:count], refs[count + 1 :]
    for i in range(count):
        for h in range(parts):
            outs[i * parts + h][...] = ins[i][0, :, h * cols : (h + 1) * cols]


def pack_weights(count, at, *refs):
    for i in range(count):
        refs[count + i][...] = refs[i][0]


def matrices(nodes, owners, capacity, at, *refs):
    infos, (mine, other, stats) = refs[:nodes], refs[nodes:]
    tokens, slots = mine.shape[1:]
    names = lax.broadcasted_iota(jnp.int32, (8, tokens), 0)
    row = lax.broadcasted_iota(jnp.int32, (tokens, tokens), 0)
    col = lax.broadcasted_iota(jnp.int32, (tokens, tokens), 1)
    earlier = (row < col).astype(f32).astype(bf16)
    slot = lax.broadcasted_iota(jnp.int32, (8, slots), 1)
    group = lax.broadcasted_iota(jnp.int32, (8, slots), 0)
    expand = ((slot >= group * capacity) & (slot < (group + 1) * capacity)).astype(f32).astype(bf16)
    place = lax.broadcasted_iota(jnp.int32, (tokens, slots), 1)
    rank = place
    for q in range(1, EXP_DEV):
        rank = jnp.where(place >= q * capacity, place - q * capacity, rank)
    rank = rank.astype(f32)
    index = lax.broadcasted_iota(jnp.int32, (owners, tokens), 0) * EXP_DEV
    low, high = index.astype(f32), (index + EXP_DEV).astype(f32)
    counts = jnp.zeros((owners, tokens), f32)
    mass = jnp.zeros((owners, tokens), f32)
    for k in range(nodes):
        ids = [infos[k][j : j + 1, :] for j in range(TOP)]
        gates = [infos[k][TOP + j : TOP + j + 1, :] for j in range(TOP)]
        for j in range(TOP):
            inside = (ids[j] >= low) & (ids[j] < high)
            counts = counts + jnp.where(inside, 1.0, 0.0)
            mass = mass + jnp.where(inside, gates[j], 0.0)
        for out, base in ((mine, at[0]), (other, at[1])):
            name = jnp.where(names < EXP_DEV, names + base, -1).astype(f32)
            hit = jnp.zeros((8, tokens), f32)
            gate = jnp.zeros((8, tokens), f32)
            for j in range(TOP):
                same = ids[j] == name
                hit = hit + jnp.where(same, 1.0, 0.0)
                gate = gate + jnp.where(same, gates[j], 0.0)
            before = jnp.dot(hit.astype(bf16), earlier, preferred_element_type=f32)
            key = jnp.where(hit > 0, before, -1.0).astype(bf16)
            across = (((0,), (0,)), ((), ()))
            wide_key = lax.dot_general(key, expand, across, preferred_element_type=f32)
            wide_gate = lax.dot_general(
                gate.astype(bf16), expand, across, preferred_element_type=f32
            )
            out[k] = jnp.where(wide_key == rank, wide_gate, 0.0).astype(bf16)
    stats[:owners] = jnp.broadcast_to(jnp.sum(counts, axis=1, keepdims=True), (owners, LANES))
    stats[owners:] = jnp.broadcast_to(jnp.sum(mass, axis=1, keepdims=True), (owners, LANES))


def combine(h, cols, at, mine, other, rows, swapped, out):
    out[...] = (
        jnp.dot(mine[0], rows[0], preferred_element_type=f32)
        + jnp.dot(other[0], swapped[...], preferred_element_type=f32)
    ).astype(out.dtype)


def combine_last(at, mine, other, rows, swapped, residual, out):
    out[...] = (
        residual[...].astype(f32)
        + jnp.dot(mine[0], rows[0], preferred_element_type=f32)
        + jnp.dot(other[0], swapped[...], preferred_element_type=f32)
    )


def project(latent_width, terms, carried, at, *refs):
    base, adds = refs[0], refs[1 : 1 + terms]
    gain, down = refs[1 + terms : 3 + terms]
    rest = refs[3 + terms :]
    total = base[...]
    for a in adds:
        total = total + a[...].astype(f32)
    stream = total.astype(bf16)
    wide = stream.astype(f32)
    latent = jnp.dot((wide * gain[...]).astype(bf16), down[...], preferred_element_type=f32)
    squares = jnp.broadcast_to(jnp.sum(wide * wide, axis=1, keepdims=True), (latent.shape[0], LANES))
    if carried:
        latent = latent + rest[0][:, :latent_width]
        squares = squares + rest[0][:, latent_width:]
    out, sums = rest[-2:]
    out[...] = stream
    sums[:, :latent_width] = latent
    sums[:, latent_width:] = squares


def final(model_width, latent_width, half, at, low, high, streams_gain, *refs):
    pass


def shards(
    expert_rows,
    expert_ids,
    gate_weights,
    residual,
    norm_gain,
    down_projection_weight,
    latent_norm_gain,
    up_projection_weight,
):
    owners = lax.axis_size("expert")
    tensors = lax.axis_size("tensor")
    rows = expert_rows[0]
    slots, width = rows.shape[1:]
    tokens = expert_ids.shape[0]
    capacity = slots // EXP_DEV
    model_width = width * tensors
    lat_cols = down_projection_weight.shape[1]
    latent_width = lat_cols * tensors
    nodes = owners // 2
    me = lax.axis_index("expert")
    x, z = me % 2, me // 2
    shard = lax.axis_index("tensor")
    parts = 2 if width % 256 == 0 else 1
    cols = width // parts
    swap = [(i, i ^ 1) for i in range(owners)]
    order = visit_order(nodes)
    dest = [jnp.asarray(order[:, i])[z] for i in range(nodes)]

    def scalars(*values):
        return jnp.stack([jnp.asarray(v, jnp.int32) for v in values])

    piece_out = jax.ShapeDtypeStruct((slots, cols), bf16)
    info, *first = call(
        functools.partial(pack_first, parts, cols),
        scalars(2 * dest[0] + 1 - x),
        [
            whole((TOP, tokens)),
            whole((TOP, tokens)),
            pl.BlockSpec((1, slots, width), lambda g, at: (at[0], 0, 0)),
        ],
        [jax.ShapeDtypeStruct((2 * TOP, tokens), f32)] + [piece_out] * parts,
        (expert_ids.T, gate_weights.T, rows),
        cost(1e6, 2 * slots * width * 2),
        "pack_first",
    )
    infos = [info]
    for k in range(1, nodes):
        shift = [(2 * i + j, 2 * ((i + k) % nodes) + j) for i in range(nodes) for j in range(2)]
        infos.append(lax.ppermute(info, "expert", shift))
    count = nodes - 1
    later = call(
        functools.partial(pack_rest, parts, cols, count),
        scalars(*[2 * dest[i] + 1 - x for i in range(1, nodes)]),
        [
            pl.BlockSpec((1, slots, width), lambda g, at, i=i: (at[i], 0, 0))
            for i in range(count)
        ]
        + [pl.BlockSpec(memory_space=pl.ANY)],
        [piece_out] * (count * parts),
        (rows,) * count + (info,),
        cost(4e6, 2 * count * slots * width * 2),
        "pack_rest",
    )
    outgoing = list(first) + list(later)
    swapped = {}
    for i in range(nodes):
        for h in range(parts):
            swapped[i, h] = lax.ppermute(outgoing[i * parts + h], "expert", swap)

    blocks = down_projection_weight.reshape(tensors, width, lat_cols)
    others = tensors - 1
    sent = call(
        functools.partial(pack_weights, others),
        scalars(*[(shard + k) % tensors for k in range(1, tensors)]),
        [
            pl.BlockSpec((1, width, lat_cols), lambda g, at, i=i: (at[i], 0, 0))
            for i in range(others)
        ],
        [jax.ShapeDtypeStruct((width, lat_cols), bf16)] * others,
        (blocks,) * others,
        cost(1e6, 2 * others * width * lat_cols * 2),
        "pack_weights",
    )
    held = [lax.dynamic_index_in_dim(blocks, shard, 0, keepdims=False)]
    for k in range(1, tensors):
        ring = [(i, (i + k) % tensors) for i in range(tensors)]
        held.append(lax.ppermute(sent[k - 1], "tensor", ring))
    stacked = jnp.stack(held)
    down = jnp.concatenate(
        [
            lax.dynamic_index_in_dim(stacked, (shard - c) % tensors, 0, keepdims=False)
            for c in range(tensors)
        ],
        axis=1,
    )

    both = jax.ShapeDtypeStruct((nodes, tokens, slots), bf16)
    mine, other, stats = call(
        functools.partial(matrices, nodes, owners, capacity),
        scalars((2 * z + x) * EXP_DEV, (2 * z + 1 - x) * EXP_DEV),
        [whole((2 * TOP, tokens))] * nodes,
        [both, both, jax.ShapeDtypeStruct((2 * owners, LANES), f32)],
        infos,
        cost(nodes * 2e7, nodes * tokens * slots * 4),
        "matrices",
    )
    stats = stats + lax.ppermute(stats, "expert", swap)
    total_tokens = float(tokens * owners)
    balance_loss = (
        owners
        * jnp.sum(stats[:owners, 0] * stats[owners:, 0])
        / (TOP * total_tokens * total_tokens)
    )

    def combine_specs(h):
        by_line = pl.BlockSpec((1, tokens, slots), lambda g, at: (at[0], 0, 0))
        return [
            by_line,
            by_line,
            pl.BlockSpec((1, slots, cols), lambda g, at: (at[1], 0, h)),
            whole((slots, cols)),
        ]

    def combine_scalars(i):
        return scalars((z - dest[i]) % nodes, 2 * dest[i] + x)

    work = cost(4 * tokens * slots * cols, 2 * (3 * slots * cols + tokens * (slots + cols)))
    partial = {}
    for i in range(nodes - 1):
        for h in range(parts):
            (partial[i, h],) = call(
                functools.partial(combine, h, cols),
                combine_scalars(i),
                combine_specs(h),
                [jax.ShapeDtypeStruct((tokens, cols), bf16)],
                (mine, other, rows, swapped[i, h]),
                work,
                "combine",
            )

    def position(s, upward):
        table = np.zeros(nodes, np.int32)
        for node in range(nodes):
            d = node + nodes - s if upward else node - nodes + s
            if 0 <= d < nodes:
                table[node] = list(order[node]).index(d)
        return table

    arrived = {}
    for s in range(1, nodes):
        for h in range(parts):
            for upward in (True, False):
                table = position(s, upward)
                top = int(table.max()) + 1
                value = pick([partial[i, h] for i in range(top)], jnp.asarray(table)[z])
                if s > 1:
                    value = (value.astype(f32) + arrived[h, upward].astype(f32)).astype(bf16)
                senders = range(s) if upward else range(nodes - s, nodes)
                step = 1 if upward else -1
                perm = [
                    (2 * i + j, 2 * (i + step) + j)
                    for i in senders
                    for j in range(2)
                    if 0 <= i + step < nodes
                ]
                arrived[h, upward] = lax.ppermute(value, "expert", perm)

    streams, sums = [], None
    gain_row = norm_gain.reshape(1, width)
    for h in range(parts):
        (base,) = call(
            combine_last,
            combine_scalars(nodes - 1),
            combine_specs(h) + [pl.BlockSpec((tokens, cols), lambda g, at: (0, h))],
            [jax.ShapeDtypeStruct((tokens, cols), f32)],
            (mine, other, rows, swapped[nodes - 1, h], residual),
            work,
            "combine_last",
        )
        adds = [arrived[h, upward] for upward in (True, False)] if nodes > 1 else []
        carried = [] if sums is None else [sums]
        stream, sums = call(
            functools.partial(project, latent_width, len(adds), len(carried)),
            scalars(0),
            [whole((tokens, cols))] * (1 + len(adds))
            + [
                pl.BlockSpec((1, cols), lambda g, at, h=h: (0, h)),
                pl.BlockSpec((cols, latent_width), lambda g, at, h=h: (h, 0)),
            ]
            + [whole((tokens, latent_width + LANES))] * len(carried),
            [
                jax.ShapeDtypeStruct((tokens, cols), bf16),
                jax.ShapeDtypeStruct((tokens, latent_width + LANES), f32),
            ],
            (base, *adds, gain_row, down, *carried),
            cost(2 * tokens * cols * latent_width, tokens * cols * 10),
            "project",
        )
        streams.append(stream)

    half = tokens // 2
    low = shard % 2 == 0

    def tensor_swap(value, bit):
        return lax.ppermute(value, "tensor", [(i, i ^ bit) for i in range(tensors)])

    top_half, bottom_half = sums[:half], sums[half:]
    total = jnp.where(low, top_half, bottom_half) + tensor_swap(
        jnp.where(low, bottom_half, top_half), 1
    )
    bit = 2
    while bit < tensors:
        squares = total[:, latent_width:]
        upper = squares.astype(bf16)
        lower = (squares - upper.astype(f32)).astype(bf16)
        got = tensor_swap(
            jnp.concatenate(
                [
                    total[:, :latent_width].astype(bf16),
                    jnp.where(jnp.arange(LANES)[None, :] % 2 == 0, upper, lower),
                ],
                axis=1,
            ),
            bit,
        ).astype(f32)
        squares = squares + got[:, latent_width : latent_width + 1] + got[:, latent_width + 1 : latent_width + 2]
        total = jnp.concatenate([total[:, :latent_width] + got[:, :latent_width], squares], axis=1)
        bit *= 2
    row_scale = lax.rsqrt(total[:, latent_width : latent_width + 1] / model_width + EPSILON)
    latent = total[:, :latent_width] * row_scale
    mean = jnp.mean(latent * latent, axis=1, keepdims=True)
    lat_normed = (latent * lax.rsqrt(mean + EPSILON) * latent_norm_gain[None, :]).astype(bf16)
    other_lat = tensor_swap(lat_normed, 1)
    scale_row = row_scale.reshape(1, half)
    other_scale = tensor_swap(scale_row, 1)
    latent_full = jnp.concatenate(
        [jnp.where(low, lat_normed, other_lat), jnp.where(low, other_lat, lat_normed)], axis=0
    )
    scale_full = jnp.concatenate(
        [jnp.where(low, scale_row, other_scale), jnp.where(low, other_scale, scale_row)], axis=1
    ).reshape(tokens, 1)
    keys_values = jnp.dot(latent_full, up_projection_weight, preferred_element_type=f32).astype(bf16)
    stream = jnp.concatenate(streams, axis=1).astype(f32)
    normed = (stream * scale_full * norm_gain[None, :]).astype(bf16)
    return (keys_values, normed, balance_loss)


def solution(mesh):
    placed = (
        P("expert", None, None, "tensor"),
        P("expert", None),
        P("expert", None),
        P("expert", "tensor"),
        P("tensor"),
        P(None, "tensor"),
        P(),
        P(None, "tensor"),
    )
    return jax.shard_map(
        shards,
        mesh=mesh,
        in_specs=placed,
        out_specs=(P("expert", "tensor"), P("expert", "tensor"), P()),
        check_vma=False,
    )
```
